32 devices in a mesh: tau: 4 (over z), row: 4 (over y, core), col: 2 (over x).
Axes of the slice: x: 2, y: 2, z: 4, core: 2. Of those that a mesh axis runs over, the one named last changes fastest.
Arguments:
- occupied: bfloat16 [4, 1024, 8192], P('tau', 'row', 'col'), may hold values from -6 to 6
- virtual_green: bfloat16 [4, 8192, 2048], P('tau', 'row', 'col'), may hold values from -0.0625 to 0.0625
- occ_mask: int32 [8, 64], P('row', 'col'), may hold values 0 or 1
- virt_mask: int32 [64, 16], P('row', 'col'), may hold values 0 or 1
- chi_mask: int32 [8, 16], P('row', 'col'), may hold values 0 or 1
- cosine_weights: float32 [4, 4], replicated, may hold values from -3 to 3
Outputs:
- chi_freq: float32 [4, 1024, 2048], P(None, ('row', 'tau'), 'col')
The draws below stay inside these ranges and needn't reach their ends.
All inputs are finite; a program needn't handle non-finite values. No bound on the sum of `occ_mask` or of `virt_mask` or of `chi_mask` on one device may be relied on, other than what follows from the above.
Results may differ from the reference program's by a relative error of at most 0.0029.
Values may be sent and summed in bfloat16 or wider, within the bound.
No kernel may reach another device: no remote copies, remote signals or barrier semaphores. Data moves between devices by JAX's collectives and lax.ppermute only.
A program may use at most 64 MiB of HBM per device.

```python
import jax
import jax.numpy as jnp
from jax import lax

N = 8192
BLOCK = 128
ROWS = 1024
COLS = 2048
TAU = 4
FREQ = 4


def with_ends(values, rng, smallest, largest):
    longest = values.shape.index(max(values.shape))
    spots = []
    for shift in (0, 1):
        where = [jax.random.randint(jax.random.fold_in(rng, axis), (), 0, length) for axis, length in enumerate(values.shape)]
        where[longest] = (where[longest] + shift) % values.shape[longest]
        spots.append(tuple(where))
    return values.at[spots[0]].set(smallest).at[spots[1]].set(largest)


def shard_levels(stream_key, dims, split, low, high):
    factor_of = 1.0
    for dim, blocks in split:
        steps = jax.random.uniform(jax.random.fold_in(jax.random.fold_in(stream_key, 6), dim), (blocks,), jnp.float32, low / len(split), high / len(split))
        factor_of = factor_of * jnp.repeat(jnp.exp(steps), dims[dim] // blocks).reshape((-1,) + (1,) * (len(dims) - 1 - dim))
    return factor_of


def centred(rng, extent, deviation, most, split=(), kind=jnp.bfloat16):
    factor_of = shard_levels(rng, extent, split, -0.22, 0.18) if split else 1.0
    values = jax.random.normal(rng, extent, jnp.float32) * deviation * factor_of
    return jnp.minimum(jnp.maximum(values, -most), most).astype(kind)


def setup_inputs(seed: int = 0) -> dict:
    seeds = jax.random.split(jax.random.key(seed), 7)
    return {
        "occupied": centred(seeds[0], (TAU, ROWS, N), 1.0, 6.0, ((0, 4), (1, 4), (2, 2))),
        "virtual_green": centred(seeds[1], (TAU, N, COLS), N ** -0.5, 0.0625, ((0, 4), (1, 4), (2, 2))),
        "occ_mask": with_ends((jax.random.randint(seeds[2], (ROWS // BLOCK, N // BLOCK), 0, 4) < 3).astype(jnp.int32), jax.random.fold_in(seeds[2], 1), 0, 1),
        "virt_mask": with_ends((jax.random.randint(seeds[3], (N // BLOCK, COLS // BLOCK), 0, 4) < 3).astype(jnp.int32), jax.random.fold_in(seeds[3], 1), 0, 1),
        "chi_mask": with_ends((jax.random.randint(seeds[4], (ROWS // BLOCK, COLS // BLOCK), 0, 3) < 2).astype(jnp.int32), jax.random.fold_in(seeds[4], 1), 0, 1),
        "cosine_weights": centred(seeds[5], (FREQ, TAU), 0.5, 3.0, (), jnp.float32),
    }


def expand_mask(values, flags):
    block_rows = values.shape[0] // flags.shape[0]
    block_cols = values.shape[1] // flags.shape[1]
    shaped = values.reshape(flags.shape[0], block_rows, flags.shape[1], block_cols)
    masked = shaped * flags.astype(values.dtype)[:, None, :, None]
    return masked.reshape(values.shape)


def reference(occupied, virtual_green, occ_mask, virt_mask, chi_mask, cosine_weights):
    def one_time(pair):
        occ_slab, virt_slab = pair
        product = jnp.dot(expand_mask(occ_slab, occ_mask), expand_mask(virt_slab, virt_mask), preferred_element_type=jnp.float32)
        return expand_mask(product, chi_mask).astype(jnp.bfloat16)

    chi_tau = lax.map(one_time, (occupied, virtual_green))
    return jnp.einsum("kt,tij->kij", cosine_weights.astype(jnp.float32), chi_tau.astype(jnp.float32), precision=lax.Precision.HIGHEST)
```

```python
import jax
import jax.numpy as jnp
from jax import lax
from jax.experimental import pallas as pl
from jax.experimental.pallas import tpu as pltpu
from jax.sharding import PartitionSpec as P


SMEM = pl.BlockSpec(memory_space=pltpu.SMEM)
VMEM = pl.BlockSpec(memory_space=pltpu.VMEM)
ANY = pl.BlockSpec(memory_space=pl.ANY)
PARAMS = pltpu.CompilerParams(vmem_limit_bytes=24 << 20)


def in_hbm(x):
    return pltpu.with_memory_space_constraint(x, pltpu.HBM)


def resident(x):
    return pltpu.with_memory_space_constraint(x, pltpu.VMEM)


def slab_of(occ, flags, place, share, step, taus, group):
    full = occ.shape[1]
    blocks = flags.shape[1]
    wide = full // blocks
    tall = occ.shape[0] // flags.shape[0]
    sub = min(share, tall)

    def body(place_ref, flags_ref, occ_ref, out_ref):
        first = (place_ref[0] + 1 + step) % taus * share
        turn = place_ref[1] * (blocks // group)
        for low in range(0, share, sub):
            line = (first + low) // tall
            for block in range(blocks):
                source = (block + turn) % blocks
                keep = flags_ref[line, source] != 0
                values = occ_ref[low : low + sub, pl.ds(pl.multiple_of(source * wide, wide), wide)]
                out_ref[low : low + sub, block * wide : (block + 1) * wide] = jnp.where(keep, values, jnp.zeros_like(values))

    return pl.pallas_call(
        body,
        grid_spec=pltpu.PrefetchScalarGridSpec(
            num_scalar_prefetch=2,
            grid=(1,),
            in_specs=[pl.BlockSpec((share, full), lambda _, at, flags: ((at[0] + 1 + step) % taus, 0))],
            out_specs=pl.BlockSpec((share, full), lambda _, at, flags: (0, 0)),
        ),
        out_shape=jax.ShapeDtypeStruct((share, full), occ.dtype),
        compiler_params=PARAMS,
        name="slab",
    )(place, in_hbm(flags), in_hbm(occ))


def loaded(virts, flags, after):
    rows, width = virts[0].shape
    lines, blocks = flags[0].shape
    tall, wide = rows // lines, width // blocks
    near = len(virts)
    batch = 4 if lines % 4 == 0 else 1

    def body(*refs):
        out_ref = refs[-1]
        for which in range(near):
            for low in range(batch):
                line = pl.program_id(0) * batch + low
                for block in range(blocks):
                    at = slice(block * wide, (block + 1) * wide)
                    keep = refs[which][line, block] != 0
                    values = refs[near + which][low * tall : (low + 1) * tall, at]
                    out_ref[which, pl.ds(pl.multiple_of(line * tall, tall), tall), at] = jnp.where(keep, values, jnp.zeros_like(values))

    return pl.pallas_call(
        body,
        grid=(lines // batch,),
        in_specs=[SMEM] * near + [pl.BlockSpec((batch * tall, width), lambda i: (i, 0))] * near + [ANY] * len(after),
        out_specs=VMEM,
        out_shape=pltpu.VMEM((near, rows, width), virts[0].dtype),
        compiler_params=PARAMS,
        name="virt",
    )(*flags, *[in_hbm(virt) for virt in virts], *after)


def products(blocks, slab, virts, place):
    share = blocks[0].shape[0]
    near, depth, width = virts.shape
    count = len(blocks)

    def body(*refs):
        place_ref, slab_ref, block_refs, virt_ref = refs[0], refs[1], refs[2 : 2 + count], refs[2 + count]
        outs = refs[3 + count : -1]
        scratch = refs[-1]
        local = jnp.where(place_ref[2] == 0, slab_ref[...], block_refs[0][...])
        rows = jnp.concatenate([local] + [ref[...] for ref in block_refs[1:]], axis=0)
        total = jnp.dot(rows[:, :depth], virt_ref[0], preferred_element_type=jnp.float32)
        for at in range(1, near):
            total += jnp.dot(rows[:, at * depth : (at + 1) * depth], virt_ref[at], preferred_element_type=jnp.float32)
        for at in range(count):
            scratch[at] = total[at * share : (at + 1) * share]
        mine = place_ref[2]
        outs[0][...] = scratch[mine]
        for shift in range(1, count):
            outs[shift][...] = scratch[(mine + shift) % count].astype(jnp.bfloat16)

    return pl.pallas_call(
        body,
        in_specs=[SMEM] + [VMEM] * (count + 2),
        out_specs=[VMEM] * count,
        out_shape=[jax.ShapeDtypeStruct((share, width), jnp.float32)]
        + [jax.ShapeDtypeStruct((share, width), jnp.bfloat16)] * (count - 1),
        scratch_shapes=[pltpu.VMEM((count, share, width), jnp.float32)],
        compiler_params=PARAMS,
        name="products",
    )(place, slab, *blocks, resident(virts))


def combine(parts, flags, place, own, step, taus):
    share, width = parts[0].shape
    wide = width // flags.shape[1]
    tall = own // flags.shape[0]
    sub = min(share, tall)

    def body(place_ref, flags_ref, *refs):
        first = (place_ref[0] + 1 + step) % taus * share
        for low in range(0, share, sub):
            line = (first + low) // tall
            for block in range(flags.shape[1]):
                at = (slice(low, low + sub), slice(block * wide, (block + 1) * wide))
                total = refs[0][at]
                for ref in refs[1:-1]:
                    total += ref[at].astype(jnp.float32)
                keep = flags_ref[line, block] != 0
                refs[-1][at] = jnp.where(keep, total, 0.0).astype(jnp.bfloat16)

    return pl.pallas_call(
        body,
        in_specs=[SMEM, SMEM] + [VMEM] * len(parts),
        out_specs=VMEM,
        out_shape=jax.ShapeDtypeStruct((share, width), jnp.bfloat16),
        compiler_params=PARAMS,
        name="combine",
    )(place, flags, *parts)


def transform(parts, moved, flags, weights, place, own):
    share, width = parts[0].shape
    wide = width // flags.shape[1]
    tall = own // flags.shape[0]
    sub = min(share, tall)
    count, taus = len(parts), len(moved) + 1
    freqs = weights.shape[0]

    def body(place_ref, flags_ref, weights_ref, *refs):
        tau, freq = place_ref[0], pl.program_id(0)
        out_ref, own_ref = refs[-2], refs[-1]

        @pl.when(freq == 0)
        def _():
            for low in range(0, share, sub):
                line = (tau * share + low) // tall
                for block in range(flags.shape[1]):
                    at = (slice(low, low + sub), slice(block * wide, (block + 1) * wide))
                    total = refs[0][at]
                    for ref in refs[1:count]:
                        total += ref[at].astype(jnp.float32)
                    keep = flags_ref[line, block] != 0
                    own_ref[at] = jnp.where(keep, total, 0.0).astype(jnp.bfloat16).astype(jnp.float32)

        total = weights_ref[freq, tau] * own_ref[...]
        for step in range(taus - 1):
            total += weights_ref[freq, (tau + taus - 1 - step) % taus] * refs[count + step][...].astype(jnp.float32)
        out_ref[0] = total

    return pl.pallas_call(
        body,
        grid=(freqs,),
        in_specs=[SMEM] * 3 + [VMEM] * (count + taus - 1),
        out_specs=pl.BlockSpec((1, share, width), lambda k: (k, 0, 0)),
        out_shape=jax.ShapeDtypeStruct((freqs, share, width), jnp.float32),
        scratch_shapes=[pltpu.VMEM((share, width), jnp.float32)],
        compiler_params=PARAMS,
        name="transform",
    )(place, flags, weights, *parts, *moved)


def solution(mesh):
    taus, rows, cols = mesh.shape["tau"], mesh.shape["row"], mesh.shape["col"]
    group = rows // cols
    everywhere = ("tau", "row", "col")

    def place_of(tau, row, col):
        return (tau * rows + row) * cols + col

    def route(target_of):
        return [
            (place_of(tau, row, col), place_of(*target_of(tau, row, col)))
            for tau in range(taus)
            for row in range(rows)
            for col in range(cols)
        ]

    def spread(far):
        pairs = []
        for tau in range(taus):
            for row in range(rows):
                for col in range(cols):
                    home, core = row // group, row % group
                    source = ((col + far) % cols) * group + core
                    if (source, home) != (row, col):
                        pairs.append((place_of(tau, source, home), place_of(tau, row, col)))
        return pairs

    def within(shift):
        return route(lambda tau, row, col: (tau, row // group * group + (row + shift) % group, col))

    def across(shift):
        return route(lambda tau, row, col: (tau, (row + shift * group) % rows, col))

    def through(shift):
        return route(lambda tau, row, col: ((tau + shift) % taus, row, col))

    def shards(occupied, virtual_green, occ_mask, virt_mask, chi_mask, cosine_weights):
        tau, row, col = (lax.axis_index(name) for name in everywhere)
        home, core = row // group, row % group
        occ = occupied[0]
        own = occ.shape[0]
        share = own // taus
        place = jnp.stack([tau, core, (home - col) % cols]).astype(jnp.int32)

        blocks, slabs = [], []
        for step in range(taus):
            slab = slab_of(occ, occ_mask, place, share, step, taus, group)
            slabs.append(slab)
            sent = {far: lax.ppermute(slab, everywhere, spread(far)) for far in [*range(1, cols), 0]}
            blocks.append([sent[far] for far in range(cols)])

        gathered = [virtual_green[0]] + [lax.ppermute(virtual_green[0], everywhere, within(-near)) for near in range(1, group)]
        flags = [virt_mask] + [lax.ppermute(virt_mask, everywhere, within(-near)) for near in range(1, group)]
        virts = loaded(gathered, flags, slabs)

        moved = []
        for step in range(taus):
            results = products(blocks[step], slabs[step], virts, place)
            parts = [results[0]] + [
                lax.ppermute(sent, everywhere, across(shift)) for shift, sent in enumerate(results[1:], 1)
            ]
            if step + 1 < taus:
                chi = combine(parts, chi_mask, place, own, step, taus)
                moved.append(lax.ppermute(chi, everywhere, through(step + 1)))
        return transform(parts, moved, chi_mask, cosine_weights, place, own)

    placed = (
        P("tau", "row", "col"),
        P("tau", "row", "col"),
        P("row", "col"),
        P("row", "col"),
        P("row", "col"),
        P(),
    )
    return jax.shard_map(
        shards,
        mesh=mesh,
        in_specs=placed,
        out_specs=P(None, ("row", "tau"), "col"),
        check_vma=False,
    )
```

```python
import jax
import jax.numpy as jnp
from jax import lax
from jax.experimental import pallas as pl
from jax.experimental.pallas import tpu as pltpu
from jax.sharding import PartitionSpec as P


SHIFTS = (3, 2, 1)
FIRST = 2

SMEM = pl.BlockSpec(memory_space=pltpu.SMEM)
VMEM = pl.BlockSpec(memory_space=pltpu.VMEM)
ANY = pl.BlockSpec(memory_space=pl.ANY)
PARAMS = pltpu.CompilerParams(vmem_limit_bytes=24 << 20)


def peer(tau, step, taus):
    return tau ^ step if taus & (taus - 1) == 0 else (tau + step) % taus


def origin(tau, step, taus):
    return tau ^ step if taus & (taus - 1) == 0 else (tau + taus - step) % taus


def in_hbm(x):
    return pltpu.with_memory_space_constraint(x, pltpu.HBM)


def resident(x):
    return pltpu.with_memory_space_constraint(x, pltpu.VMEM)


def slab_of(occ, flags, place, piece, taus, after, where):
    step, offset, size = piece
    full, blocks = occ.shape[1], flags.shape[1]
    share = occ.shape[0] // taus
    wide = full // blocks
    tall = occ.shape[0] // flags.shape[0]
    sub = min(size, tall)

    def body(place_ref, flags_ref, occ_ref, *rest):
        out_ref = rest[-1]
        first = peer(place_ref[0], step, taus) * share + offset
        for low in range(0, size, sub):
            line = (first + low) // tall
            for block in range(blocks):
                at = (slice(low, low + sub), slice(block * wide, (block + 1) * wide))
                values = occ_ref[at]
                out_ref[at] = jnp.where(flags_ref[line, block] != 0, values, jnp.zeros_like(values))

    return pl.pallas_call(
        body,
        grid_spec=pltpu.PrefetchScalarGridSpec(
            num_scalar_prefetch=2,
            grid=(1,),
            in_specs=[pl.BlockSpec((size, full), lambda _, at, flags: ((peer(at[0], step, taus) * share + offset) // size, 0))]
            + [ANY] * len(after),
            out_specs=pl.BlockSpec((size, full), lambda _, at, flags: (0, 0)),
        ),
        out_shape=jax.ShapeDtypeStruct((size, full), occ.dtype),
        compiler_params=PARAMS,
        name="slab",
    )(place, in_hbm(flags), where(occ), *after)


def first_slabs(occ, flags, place, shifts, taus, pieces=0):
    full, blocks = occ.shape[1], flags.shape[1]
    share = occ.shape[0] // taus
    wide = full // blocks
    tall = occ.shape[0] // flags.shape[0]
    sub = min(share, tall)
    count = len(shifts)

    def body(place_ref, flags_hbm, occ_hbm, *refs):
        outs, (flags_ref, rows, flag_sem, sems) = refs[: count + pieces], refs[count + pieces :]
        starts = [pl.multiple_of(peer(place_ref[0], shift, taus) * share, share) for shift in shifts]
        copies = [pltpu.make_async_copy(occ_hbm.at[pl.ds(start, share)], rows.at[at], sems.at[at]) for at, start in enumerate(starts)]
        flag_copy = pltpu.make_async_copy(flags_hbm, flags_ref, flag_sem)
        for copy in [*copies, flag_copy]:
            copy.start()
        flag_copy.wait()
        for which, copy in enumerate(copies):
            copy.wait()
            for low in range(0, share, sub):
                line = (starts[which] + low) // tall
                for block in range(blocks):
                    lines, across = slice(low, low + sub), slice(block * wide, (block + 1) * wide)
                    values = rows[which, lines, across]
                    values = jnp.where(flags_ref[line, block] != 0, values, jnp.zeros_like(values))
                    outs[which][lines, across] = values
                    if pieces and which + 1 == count:
                        per = blocks // pieces
                        left = block % per * wide
                        outs[count + block // per][lines, left : left + wide] = values

    return pl.pallas_call(
        body,
        in_specs=[SMEM, ANY, ANY],
        out_specs=[VMEM] * (count + pieces),
        out_shape=[jax.ShapeDtypeStruct((share, full), occ.dtype)] * count
        + [jax.ShapeDtypeStruct((share, full // max(pieces, 1)), occ.dtype)] * pieces,
        scratch_shapes=[
            pltpu.SMEM(flags.shape, flags.dtype),
            pltpu.VMEM((count, share, full), occ.dtype),
            pltpu.SemaphoreType.DMA(()),
            pltpu.SemaphoreType.DMA((count,)),
        ],
        compiler_params=PARAMS,
        name="slabs",
    )(place, in_hbm(flags), in_hbm(occ))


def loaded(virts, flags, place, after):
    rows, width = virts[0].shape
    lines, blocks = flags[0].shape
    tall, wide = rows // lines, width // blocks
    near = len(virts)
    batch = 4 if lines % 4 == 0 else 1

    def body(*refs):
        place_ref, refs = refs[0], refs[1:]
        out_ref = refs[-1]
        for which in range(near):
            slot = (place_ref[1] + which) % near
            for low in range(batch):
                line = pl.program_id(0) * batch + low
                for block in range(blocks):
                    at = slice(block * wide, (block + 1) * wide)
                    keep = refs[which][line, block] != 0
                    values = refs[near + which][low * tall : (low + 1) * tall, at]
                    out_ref[slot, pl.ds(pl.multiple_of(line * tall, tall), tall), at] = jnp.where(keep, values, jnp.zeros_like(values))

    return pl.pallas_call(
        body,
        grid=(lines // batch,),
        in_specs=[SMEM] * (near + 1) + [pl.BlockSpec((batch * tall, width), lambda i: (i, 0))] * near + [ANY] * len(after),
        out_specs=VMEM,
        out_shape=pltpu.VMEM((near, rows, width), virts[0].dtype),
        compiler_params=PARAMS,
        name="virt",
    )(place, *flags, *[in_hbm(virt) for virt in virts], *after)


def products(blocks, slab, virts, place, after):
    share = blocks[0].shape[0]
    near, depth, width = virts.shape
    count = len(blocks)

    def body(*refs):
        place_ref, slab_ref, block_refs, virt_ref = refs[0], refs[1], refs[2 : 2 + count], refs[2 + count]
        outs = refs[3 + count + len(after) : -1]
        scratch = refs[-1]
        local = jnp.where(place_ref[2] == 0, slab_ref[...], block_refs[0][...])
        rows = jnp.concatenate([local] + [ref[...] for ref in block_refs[1:]], axis=0)
        total = jnp.dot(rows[:, :depth], virt_ref[0], preferred_element_type=jnp.float32)
        for at in range(1, near):
            total += jnp.dot(rows[:, at * depth : (at + 1) * depth], virt_ref[at], preferred_element_type=jnp.float32)
        for at in range(count):
            scratch[at] = total[at * share : (at + 1) * share]
        mine = place_ref[2]
        outs[0][...] = scratch[mine]
        for shift in range(1, count):
            outs[shift][...] = scratch[(mine + shift) % count].astype(jnp.bfloat16)

    return pl.pallas_call(
        body,
        in_specs=[SMEM] + [VMEM] * (count + 2) + [ANY] * len(after),
        out_specs=[VMEM] * count,
        out_shape=[jax.ShapeDtypeStruct((share, width), jnp.float32)]
        + [jax.ShapeDtypeStruct((share, width), jnp.bfloat16)] * (count - 1),
        scratch_shapes=[pltpu.VMEM((count, share, width), jnp.float32)],
        compiler_params=PARAMS,
        name="products",
    )(place, slab, *blocks, resident(virts), *after)


def grouped(items, virts, place):
    share, full = items[0][0].shape
    near, depth, width = virts.shape
    tile = min(width, 256)
    count = len(items)

    def body(place_ref, *refs):
        virt_ref, outs, rows = refs[2 * count], refs[2 * count + 1 : -1], refs[-1]
        for which in range(2):
            @pl.when((place_ref[2] == 0) == (which == 0))
            def _():
                for at in range(count):
                    rows[at * share : (at + 1) * share, :] = refs[2 * at + which][...]

        for left in range(0, width, tile):
            total = 0.0
            for at in range(near):
                total += jnp.dot(
                    rows[:, at * depth : (at + 1) * depth], virt_ref[at, :, left : left + tile], preferred_element_type=jnp.float32
                )
            for at, out in enumerate(outs):
                out[:, left : left + tile] = total[at * share : (at + 1) * share].astype(out.dtype)

    arrays = [array for first, second, _ in items for array in (first, second)]
    return pl.pallas_call(
        body,
        in_specs=[SMEM] + [VMEM] * (len(arrays) + 1),
        out_specs=[VMEM] * count,
        out_shape=[jax.ShapeDtypeStruct((share, width), kind) for _, _, kind in items],
        scratch_shapes=[pltpu.VMEM((max(count * share, 128), full), items[0][0].dtype)],
        compiler_params=PARAMS,
        name="grouped",
    )(place, *arrays, resident(virts))


def combine(parts, flags, place, own, piece, taus):
    step, offset, size = piece
    share, width = own // taus, parts[0].shape[1]
    wide = width // flags.shape[1]
    tall = own // flags.shape[0]
    sub = min(size, tall)

    def body(place_ref, flags_ref, *refs):
        first = peer(place_ref[0], step, taus) * share + offset
        for low in range(0, size, sub):
            line = (first + low) // tall
            for block in range(flags.shape[1]):
                at = (slice(low, low + sub), slice(block * wide, (block + 1) * wide))
                total = refs[0][at]
                for ref in refs[1:-1]:
                    total += ref[at].astype(jnp.float32)
                keep = flags_ref[line, block] != 0
                refs[-1][at] = jnp.where(keep, total, 0.0).astype(jnp.bfloat16)

    return pl.pallas_call(
        body,
        in_specs=[SMEM, SMEM] + [VMEM] * len(parts),
        out_specs=VMEM,
        out_shape=jax.ShapeDtypeStruct((size, width), jnp.bfloat16),
        compiler_params=PARAMS,
        name="combine",
    )(place, flags, *parts)


def transform(slabs, steps_of, flags, weights, place, own):
    share, width = slabs[0][0].shape
    taus, freqs = len(slabs), weights.shape[0]
    wide = width // flags.shape[1]
    tall = own // flags.shape[0]
    sub = min(share, tall)
    blocks = flags.shape[1]
    steps = 4 if blocks % 4 == 0 else 1
    tile = width // steps
    arrays = [part for parts in slabs for part in parts]

    def body(place_ref, flags_ref, weights_ref, *refs):
        ins, (out_hbm, out, sems) = list(refs[: len(arrays)]), refs[len(arrays) :]
        tau = place_ref[0]
        grouped_refs = [[ins.pop(0) for _ in parts] for parts in slabs]
        scale = [[weights_ref[freq, origin(tau, step, taus)] for step in steps_of] for freq in range(freqs)]
        copies = []
        for step in range(steps):
            for block in range(step * (blocks // steps), (step + 1) * (blocks // steps)):
                for low in range(0, share, sub):
                    at = (slice(low, low + sub), slice(block * wide, (block + 1) * wide))
                    keep = flags_ref[(tau * share + low) // tall, block] != 0
                    values = []
                    for parts in grouped_refs:
                        total = sum(ref[at].astype(jnp.float32) for ref in parts)
                        if len(parts) > 1:
                            total = jnp.where(keep, total, 0.0).astype(jnp.bfloat16).astype(jnp.float32)
                        values.append(total)
                    for freq in range(freqs):
                        out[(freq,) + at] = sum(scale[freq][turn] * values[turn] for turn in range(taus))
            across = slice(step * tile, (step + 1) * tile)
            copies.append(pltpu.make_async_copy(out.at[:, :, across], out_hbm.at[:, :, across], sems.at[step]))
            copies[-1].start()
        for copy in copies:
            copy.wait()

    return pl.pallas_call(
        body,
        in_specs=[SMEM] * 3 + [VMEM] * len(arrays),
        out_specs=ANY,
        out_shape=jax.ShapeDtypeStruct((freqs, share, width), jnp.float32),
        scratch_shapes=[pltpu.VMEM((freqs, share, width), jnp.float32), pltpu.SemaphoreType.DMA((steps,))],
        compiler_params=PARAMS,
        name="transform",
    )(place, flags, weights, *arrays)


def section(slab, home, virts, place, part):
    share, width = slab.shape[0], virts.shape[2]
    depth = virts.shape[1]
    tile = min(width, 256)

    def body(place_ref, slab_ref, home_ref, virt_ref, out_ref, rows):
        for which, ref in enumerate((slab_ref, home_ref)):
            left = 0 if ref.shape[1] == depth else part * depth

            @pl.when((place_ref[2] == 0) == (which == 0))
            def _():
                rows[:share, :] = ref[:, left : left + depth]

        for left in range(0, width, tile):
            total = jnp.dot(rows[...], virt_ref[part, :, left : left + tile], preferred_element_type=jnp.float32)
            out_ref[:, left : left + tile] = total[:share]

    return pl.pallas_call(
        body,
        in_specs=[SMEM] + [VMEM] * 3,
        out_specs=VMEM,
        out_shape=jax.ShapeDtypeStruct((share, width), jnp.float32),
        scratch_shapes=[pltpu.VMEM((max(share, 128), depth), slab.dtype)],
        compiler_params=PARAMS,
        name="section",
    )(place, slab, home, resident(virts))


def solution(mesh):
    taus, rows, cols = mesh.shape["tau"], mesh.shape["row"], mesh.shape["col"]
    group = rows // cols
    everywhere = ("tau", "row", "col")

    def place_of(tau, row, col):
        return (tau * rows + row) * cols + col

    def route(target_of):
        return [
            (place_of(tau, row, col), place_of(*target_of(tau, row, col)))
            for tau in range(taus)
            for row in range(rows)
            for col in range(cols)
            if target_of(tau, row, col)
        ]

    def spread(far):
        pairs = []
        for tau in range(taus):
            for row in range(rows):
                for col in range(cols):
                    home, core = row // group, row % group
                    source = ((col + far) % cols) * group + core
                    if (source, home) != (row, col):
                        pairs.append((place_of(tau, source, home), place_of(tau, row, col)))
        return pairs

    def within(shift):
        return route(lambda tau, row, col: (tau, row // group * group + (row + shift) % group, col))

    def across(shift):
        return route(lambda tau, row, col: (tau, (row + shift * group) % rows, col))

    def through(shift):
        return route(lambda tau, row, col: (peer(tau, shift, taus), row, col))

    def beside(diagonal, others):
        def target(tau, row, col):
            home, core = row // group, row % group
            if home == col:
                return (tau, row, 1 - col) if diagonal else None
            return (tau, col * group + core, col) if others else None

        return route(target)

    def turned(diagonal):
        return route(lambda tau, row, col: (tau, row, 1 - col) if (row // group == col) == diagonal else None)

    opposite = route(
        lambda tau, row, col: None if row // group == col else (tau, (1 - row // group) * group + row % group, 1 - col)
    ) if cols == 2 else None

    def shards(occupied, virtual_green, occ_mask, virt_mask, chi_mask, cosine_weights):
        tau, row, col = (lax.axis_index(name) for name in everywhere)
        home, core = row // group, row % group
        occ = occupied[0]
        own = occ.shape[0]
        share = own // taus
        place = jnp.stack([tau, core, (home - col) % cols]).astype(jnp.int32)

        def move(x, pairs):
            return lax.ppermute(x, everywhere, pairs)

        def gather_virts(after):
            gathered, flags = [virtual_green[0]], [virt_mask]
            for near in range(1, group):
                gathered.append(move(virtual_green[0], within(-near)))
                flags.append(move(virt_mask, within(-near)))
            return loaded(gathered, flags, place, after)

        if cols == 2 and taus == len(SHIFTS) + 1 and group == 2:
            pieces = [(shift, 0, share) for shift in SHIFTS] + [(0, 0, share)]
            slabs = list(first_slabs(occ, occ_mask, place, [piece[0] for piece in pieces[:FIRST]], taus))
            slabs += list(first_slabs(occ, occ_mask, place, [piece[0] for piece in pieces[FIRST:]], taus, group))
            slabs, halves = slabs[: len(pieces)], slabs[len(pieces) :]
            last = len(pieces) - 1
            virts = gather_virts(slabs)
            home_in, near_in, far_in = {}, {}, {}
            for at in range(last + 1):
                if at < 2:
                    home_in[at] = near_in[at] = move(slabs[at], beside(True, True))
                else:
                    home_in[at] = move(slabs[at] if at < last else halves[0], beside(True, False))
                    if at < last:
                        near_in[at] = move(slabs[at], beside(False, True))
                if at:
                    far_in[at] = move(slabs[at], opposite)
            ending = move(halves[1], beside(True, False))
            far_in[0] = move(near_in[0], turned(True))
            near_in[last] = move(far_in[last], turned(False))
            rounded = jnp.bfloat16

            def remote(at):
                return (near_in[at], far_in[at], rounded)

            def local(at):
                return (slabs[at], home_in[at], jnp.float32)

            remotes, locals_ = {}, {}
            remotes[1], locals_[0], locals_[1] = grouped([remote(1), local(0), local(1)], virts, place)
            remotes[0], = grouped([remote(0)], virts, place)
            remotes[2], = grouped([remote(2)], virts, place)
            remotes[3], locals_[2] = grouped([remote(3), local(2)], virts, place)
            kept = []
            for at, piece in enumerate(pieces[:last]):
                chi = combine([locals_[at], move(remotes[at], across(1))], chi_mask, place, own, piece, taus)
                kept.append([move(chi, through(piece[0]))])
            stays = [
                section(slabs[last], home_in[last], virts, place, 0),
                section(slabs[last], ending, virts, place, 1),
                move(remotes[last], across(1)),
            ]
            return transform([stays, *kept], (0,) + SHIFTS, chi_mask, cosine_weights, place, own)

        slabs, received = [], []
        pieces = [(step, 0, share) for step in [*range(1, taus), 0]]
        for at, piece in enumerate(pieces):
            slabs.append(slab_of(occ, occ_mask, place, piece, taus, [], in_hbm))
            received.append([move(slabs[at], spread(far)) for far in range(cols)])
        virts = gather_virts(slabs)
        moved = []
        for at, piece in enumerate(pieces):
            results = products(received[at], slabs[at], virts, place, [])
            parts = [results[0]] + [move(sent, across(shift)) for shift, sent in enumerate(results[1:], 1)]
            if piece[0]:
                chi = combine(parts, chi_mask, place, own, piece, taus)
                moved.append(move(chi, through(piece[0])))
        return transform([parts] + [[slab] for slab in moved], range(taus), chi_mask, cosine_weights, place, own)

    placed = (
        P("tau", "row", "col"),
        P("tau", "row", "col"),
        P("row", "col"),
        P("row", "col"),
        P("row", "col"),
        P(),
    )
    step = jax.shard_map(
        shards,
        mesh=mesh,
        in_specs=placed,
        out_specs=P(None, ("row", "tau"), "col"),
        check_vma=False,
    )
    if cols != 2 or taus != len(SHIFTS) + 1 or group != 2:
        return step
    return step
```

```python
import jax
import jax.numpy as jnp
from jax import lax
from jax.experimental import pallas as pl
from jax.experimental.pallas import tpu as pltpu
from jax.sharding import PartitionSpec as P


SHIFTS = (3, 2, 1)
FIRST = 2

SMEM = pl.BlockSpec(memory_space=pltpu.SMEM)
VMEM = pl.BlockSpec(memory_space=pltpu.VMEM)
ANY = pl.BlockSpec(memory_space=pl.ANY)
PARAMS = pltpu.CompilerParams(vmem_limit_bytes=24 << 20)


def peer(tau, step, taus):
    return tau ^ step if taus & (taus - 1) == 0 else (tau + step) % taus


def origin(tau, step, taus):
    return tau ^ step if taus & (taus - 1) == 0 else (tau + taus - step) % taus


def in_hbm(x):
    return pltpu.with_memory_space_constraint(x, pltpu.HBM)


def resident(x):
    return pltpu.with_memory_space_constraint(x, pltpu.VMEM)


def slab_of(occ, flags, place, piece, taus, after, where):
    step, offset, size = piece
    full, blocks = occ.shape[1], flags.shape[1]
    share = occ.shape[0] // taus
    wide = full // blocks
    tall = occ.shape[0] // flags.shape[0]
    sub = min(size, tall)

    def body(place_ref, flags_ref, occ_ref, *rest):
        out_ref = rest[-1]
        first = peer(place_ref[0], step, taus) * share + offset
        for low in range(0, size, sub):
            line = (first + low) // tall
            for block in range(blocks):
                at = (slice(low, low + sub), slice(block * wide, (block + 1) * wide))
                values = occ_ref[at]
                out_ref[at] = jnp.where(flags_ref[line, block] != 0, values, jnp.zeros_like(values))

    return pl.pallas_call(
        body,
        grid_spec=pltpu.PrefetchScalarGridSpec(
            num_scalar_prefetch=2,
            grid=(1,),
            in_specs=[pl.BlockSpec((size, full), lambda _, at, flags: ((peer(at[0], step, taus) * share + offset) // size, 0))]
            + [ANY] * len(after),
            out_specs=pl.BlockSpec((size, full), lambda _, at, flags: (0, 0)),
        ),
        out_shape=jax.ShapeDtypeStruct((size, full), occ.dtype),
        compiler_params=PARAMS,
        name="slab",
    )(place, in_hbm(flags), where(occ), *after)


def first_slabs(occ, flags, place, shifts, taus):
    full, blocks = occ.shape[1], flags.shape[1]
    share = occ.shape[0] // taus
    wide = full // blocks
    tall = occ.shape[0] // flags.shape[0]
    sub = min(share, tall)
    count = len(shifts)

    def body(place_ref, flags_hbm, occ_hbm, *refs):
        outs, (flags_ref, rows, flag_sem, sems) = refs[:count], refs[count:]
        starts = [pl.multiple_of(peer(place_ref[0], shift, taus) * share, share) for shift in shifts]
        copies = [pltpu.make_async_copy(occ_hbm.at[pl.ds(start, share)], rows.at[at], sems.at[at]) for at, start in enumerate(starts)]
        flag_copy = pltpu.make_async_copy(flags_hbm, flags_ref, flag_sem)
        for copy in [*copies, flag_copy]:
            copy.start()
        flag_copy.wait()
        for which, copy in enumerate(copies):
            copy.wait()
            for low in range(0, share, sub):
                line = (starts[which] + low) // tall
                for block in range(blocks):
                    lines, across = slice(low, low + sub), slice(block * wide, (block + 1) * wide)
                    values = rows[which, lines, across]
                    outs[which][lines, across] = jnp.where(flags_ref[line, block] != 0, values, jnp.zeros_like(values))

    return pl.pallas_call(
        body,
        in_specs=[SMEM, ANY, ANY],
        out_specs=[VMEM] * count,
        out_shape=[jax.ShapeDtypeStruct((share, full), occ.dtype)] * count,
        scratch_shapes=[
            pltpu.SMEM(flags.shape, flags.dtype),
            pltpu.VMEM((count, share, full), occ.dtype),
            pltpu.SemaphoreType.DMA(()),
            pltpu.SemaphoreType.DMA((count,)),
        ],
        compiler_params=PARAMS,
        name="slabs",
    )(place, in_hbm(flags), in_hbm(occ))


def loaded(virts, flags, place, after):
    rows, width = virts[0].shape
    lines, blocks = flags[0].shape
    tall, wide = rows // lines, width // blocks
    near = len(virts)
    batch = 4 if lines % 4 == 0 else 1

    def body(*refs):
        place_ref, refs = refs[0], refs[1:]
        out_ref = refs[-1]
        for which in range(near):
            slot = (place_ref[1] + which) % near
            for low in range(batch):
                line = pl.program_id(0) * batch + low
                for block in range(blocks):
                    at = slice(block * wide, (block + 1) * wide)
                    keep = refs[which][line, block] != 0
                    values = refs[near + which][low * tall : (low + 1) * tall, at]
                    out_ref[slot, pl.ds(pl.multiple_of(line * tall, tall), tall), at] = jnp.where(keep, values, jnp.zeros_like(values))

    return pl.pallas_call(
        body,
        grid=(lines // batch,),
        in_specs=[SMEM] * (near + 1) + [pl.BlockSpec((batch * tall, width), lambda i: (i, 0))] * near + [ANY] * len(after),
        out_specs=VMEM,
        out_shape=pltpu.VMEM((near, rows, width), virts[0].dtype),
        compiler_params=PARAMS,
        name="virt",
    )(place, *flags, *[in_hbm(virt) for virt in virts], *after)


def products(blocks, slab, virts, place, after):
    share = blocks[0].shape[0]
    near, depth, width = virts.shape
    count = len(blocks)

    def body(*refs):
        place_ref, slab_ref, block_refs, virt_ref = refs[0], refs[1], refs[2 : 2 + count], refs[2 + count]
        outs = refs[3 + count + len(after) : -1]
        scratch = refs[-1]
        local = jnp.where(place_ref[2] == 0, slab_ref[...], block_refs[0][...])
        rows = jnp.concatenate([local] + [ref[...] for ref in block_refs[1:]], axis=0)
        total = jnp.dot(rows[:, :depth], virt_ref[0], preferred_element_type=jnp.float32)
        for at in range(1, near):
            total += jnp.dot(rows[:, at * depth : (at + 1) * depth], virt_ref[at], preferred_element_type=jnp.float32)
        for at in range(count):
            scratch[at] = total[at * share : (at + 1) * share]
        mine = place_ref[2]
        outs[0][...] = scratch[mine]
        for shift in range(1, count):
            outs[shift][...] = scratch[(mine + shift) % count].astype(jnp.bfloat16)

    return pl.pallas_call(
        body,
        in_specs=[SMEM] + [VMEM] * (count + 2) + [ANY] * len(after),
        out_specs=[VMEM] * count,
        out_shape=[jax.ShapeDtypeStruct((share, width), jnp.float32)]
        + [jax.ShapeDtypeStruct((share, width), jnp.bfloat16)] * (count - 1),
        scratch_shapes=[pltpu.VMEM((count, share, width), jnp.float32)],
        compiler_params=PARAMS,
        name="products",
    )(place, slab, *blocks, resident(virts), *after)


def grouped(items, virts, place):
    share, full = items[0][0].shape
    near, depth, width = virts.shape
    tile = min(width, 256)
    count = len(items)

    def body(place_ref, *refs):
        virt_ref, outs, rows = refs[2 * count], refs[2 * count + 1 : -1], refs[-1]
        for which in range(2):
            @pl.when((place_ref[2] == 0) == (which == 0))
            def _():
                for at in range(count):
                    rows[at * share : (at + 1) * share, :] = refs[2 * at + which][...]

        for left in range(0, width, tile):
            total = 0.0
            for at in range(near):
                total += jnp.dot(
                    rows[:, at * depth : (at + 1) * depth], virt_ref[at, :, left : left + tile], preferred_element_type=jnp.float32
                )
            for at, out in enumerate(outs):
                out[:, left : left + tile] = total[at * share : (at + 1) * share].astype(out.dtype)

    arrays = [array for first, second, _ in items for array in (first, second)]
    return pl.pallas_call(
        body,
        in_specs=[SMEM] + [VMEM] * (len(arrays) + 1),
        out_specs=[VMEM] * count,
        out_shape=[jax.ShapeDtypeStruct((share, width), kind) for _, _, kind in items],
        scratch_shapes=[pltpu.VMEM((max(count * share, 128), full), items[0][0].dtype)],
        compiler_params=PARAMS,
        name="grouped",
    )(place, *arrays, resident(virts))


def combine(parts, flags, place, own, piece, taus):
    step, offset, size = piece
    share, width = own // taus, parts[0].shape[1]
    wide = width // flags.shape[1]
    tall = own // flags.shape[0]
    sub = min(size, tall)

    def body(place_ref, flags_ref, *refs):
        first = peer(place_ref[0], step, taus) * share + offset
        for low in range(0, size, sub):
            line = (first + low) // tall
            for block in range(flags.shape[1]):
                at = (slice(low, low + sub), slice(block * wide, (block + 1) * wide))
                total = refs[0][at]
                for ref in refs[1:-1]:
                    total += ref[at].astype(jnp.float32)
                keep = flags_ref[line, block] != 0
                refs[-1][at] = jnp.where(keep, total, 0.0).astype(jnp.bfloat16)

    return pl.pallas_call(
        body,
        in_specs=[SMEM, SMEM] + [VMEM] * len(parts),
        out_specs=VMEM,
        out_shape=jax.ShapeDtypeStruct((size, width), jnp.bfloat16),
        compiler_params=PARAMS,
        name="combine",
    )(place, flags, *parts)


def transform(slabs, steps_of, flags, weights, place, own):
    share, width = slabs[0][0].shape
    taus, freqs = len(slabs), weights.shape[0]
    wide = width // flags.shape[1]
    tall = own // flags.shape[0]
    sub = min(share, tall)
    blocks = flags.shape[1]
    steps = 4 if blocks % 4 == 0 else 1
    tile = width // steps
    arrays = [part for parts in slabs for part in parts]

    def body(place_ref, flags_ref, weights_ref, *refs):
        ins, (out_hbm, out, sems) = list(refs[: len(arrays)]), refs[len(arrays) :]
        tau = place_ref[0]
        grouped_refs = [[ins.pop(0) for _ in parts] for parts in slabs]
        scale = [[weights_ref[freq, origin(tau, step, taus)] for step in steps_of] for freq in range(freqs)]
        copies = []
        for step in range(steps):
            for block in range(step * (blocks // steps), (step + 1) * (blocks // steps)):
                for low in range(0, share, sub):
                    at = (slice(low, low + sub), slice(block * wide, (block + 1) * wide))
                    keep = flags_ref[(tau * share + low) // tall, block] != 0
                    values = []
                    for parts in grouped_refs:
                        total = sum(ref[at].astype(jnp.float32) for ref in parts)
                        if len(parts) > 1:
                            total = jnp.where(keep, total, 0.0).astype(jnp.bfloat16).astype(jnp.float32)
                        values.append(total)
                    for freq in range(freqs):
                        out[(freq,) + at] = sum(scale[freq][turn] * values[turn] for turn in range(taus))
            across = slice(step * tile, (step + 1) * tile)
            copies.append(pltpu.make_async_copy(out.at[:, :, across], out_hbm.at[:, :, across], sems.at[step]))
            copies[-1].start()
        for copy in copies:
            copy.wait()

    return pl.pallas_call(
        body,
        in_specs=[SMEM] * 3 + [VMEM] * len(arrays),
        out_specs=ANY,
        out_shape=jax.ShapeDtypeStruct((freqs, share, width), jnp.float32),
        scratch_shapes=[pltpu.VMEM((freqs, share, width), jnp.float32), pltpu.SemaphoreType.DMA((steps,))],
        compiler_params=PARAMS,
        name="transform",
    )(place, flags, weights, *arrays)


def solution(mesh):
    taus, rows, cols = mesh.shape["tau"], mesh.shape["row"], mesh.shape["col"]
    group = rows // cols
    everywhere = ("tau", "row", "col")

    def place_of(tau, row, col):
        return (tau * rows + row) * cols + col

    def route(target_of):
        return [
            (place_of(tau, row, col), place_of(*target_of(tau, row, col)))
            for tau in range(taus)
            for row in range(rows)
            for col in range(cols)
            if target_of(tau, row, col)
        ]

    def spread(far):
        pairs = []
        for tau in range(taus):
            for row in range(rows):
                for col in range(cols):
                    home, core = row // group, row % group
                    source = ((col + far) % cols) * group + core
                    if (source, home) != (row, col):
                        pairs.append((place_of(tau, source, home), place_of(tau, row, col)))
        return pairs

    def within(shift):
        return route(lambda tau, row, col: (tau, row // group * group + (row + shift) % group, col))

    def across(shift):
        return route(lambda tau, row, col: (tau, (row + shift * group) % rows, col))

    def through(shift):
        return route(lambda tau, row, col: (peer(tau, shift, taus), row, col))

    def beside(diagonal, others):
        def target(tau, row, col):
            home, core = row // group, row % group
            if home == col:
                return (tau, row, 1 - col) if diagonal else None
            return (tau, col * group + core, col) if others else None

        return route(target)

    def turned(diagonal):
        return route(lambda tau, row, col: (tau, row, 1 - col) if (row // group == col) == diagonal else None)

    opposite = route(
        lambda tau, row, col: None if row // group == col else (tau, (1 - row // group) * group + row % group, 1 - col)
    ) if cols == 2 else None

    def shards(occupied, virtual_green, occ_mask, virt_mask, chi_mask, cosine_weights):
        tau, row, col = (lax.axis_index(name) for name in everywhere)
        home, core = row // group, row % group
        occ = occupied[0]
        own = occ.shape[0]
        share = own // taus
        place = jnp.stack([tau, core, (home - col) % cols]).astype(jnp.int32)

        def move(x, pairs):
            return lax.ppermute(x, everywhere, pairs)

        def gather_virts(after):
            gathered, flags = [virtual_green[0]], [virt_mask]
            for near in range(1, group):
                gathered.append(move(virtual_green[0], within(-near)))
                flags.append(move(virt_mask, within(-near)))
            return loaded(gathered, flags, place, after)

        if cols == 2 and taus == len(SHIFTS) + 1 and group == 2:
            pieces = [(shift, 0, share) for shift in SHIFTS] + [(0, 0, share)]
            slabs = list(first_slabs(occ, occ_mask, place, [piece[0] for piece in pieces[:FIRST]], taus))
            slabs += list(first_slabs(occ, occ_mask, place, [piece[0] for piece in pieces[FIRST:]], taus))
            last = len(pieces) - 1
            virts = gather_virts(slabs)
            home_in, near_in, far_in = {}, {}, {}
            for at in range(last + 1):
                if at < 2:
                    home_in[at] = near_in[at] = move(slabs[at], beside(True, True))
                else:
                    home_in[at] = move(slabs[at], beside(True, False))
                    if at < last:
                        near_in[at] = move(slabs[at], beside(False, True))
                if at:
                    far_in[at] = move(slabs[at], opposite)
            far_in[0] = move(near_in[0], turned(True))
            near_in[last] = move(far_in[last], turned(False))
            rounded = jnp.bfloat16

            def remote(at):
                return (near_in[at], far_in[at], rounded)

            def local(at):
                return (slabs[at], home_in[at], jnp.float32)

            remotes, locals_ = {}, {}
            remotes[1], locals_[0], locals_[1] = grouped([remote(1), local(0), local(1)], virts, place)
            remotes[0], = grouped([remote(0)], virts, place)
            remotes[2], = grouped([remote(2)], virts, place)
            remotes[3], locals_[2] = grouped([remote(3), local(2)], virts, place)
            locals_[3], = grouped([local(3)], virts, place)
            kept = [[locals_[last], move(remotes[last], across(1))]]
            for at, piece in enumerate(pieces[:last]):
                chi = combine([locals_[at], move(remotes[at], across(1))], chi_mask, place, own, piece, taus)
                kept.append([move(chi, through(piece[0]))])
            return transform(kept, (0,) + SHIFTS, chi_mask, cosine_weights, place, own)

        slabs, received = [], []
        pieces = [(step, 0, share) for step in [*range(1, taus), 0]]
        for at, piece in enumerate(pieces):
            slabs.append(slab_of(occ, occ_mask, place, piece, taus, [], in_hbm))
            received.append([move(slabs[at], spread(far)) for far in range(cols)])
        virts = gather_virts(slabs)
        moved = []
        for at, piece in enumerate(pieces):
            results = products(received[at], slabs[at], virts, place, [])
            parts = [results[0]] + [move(sent, across(shift)) for shift, sent in enumerate(results[1:], 1)]
            if piece[0]:
                chi = combine(parts, chi_mask, place, own, piece, taus)
                moved.append(move(chi, through(piece[0])))
        return transform([parts] + [[slab] for slab in moved], range(taus), chi_mask, cosine_weights, place, own)

    placed = (
        P("tau", "row", "col"),
        P("tau", "row", "col"),
        P("row", "col"),
        P("row", "col"),
        P("row", "col"),
        P(),
    )
    step = jax.shard_map(
        shards,
        mesh=mesh,
        in_specs=placed,
        out_specs=P(None, ("row", "tau"), "col"),
        check_vma=False,
    )
    if cols != 2 or taus != len(SHIFTS) + 1 or group != 2:
        return step
    return step
```
